32 devices in a mesh: dp: 8 (over z, x), tp: 4 (over y, core).
Axes of the slice: x: 2, y: 2, z: 4, core: 2. Of those that a mesh axis runs over, the one named last changes fastest.
Arguments:
- queries: bfloat16 [4096, 8192], P('dp', 'tp'), parts along dimension 0, may hold values from -200 to 200
- new_keys: bfloat16 [4096, 1024], P('dp', 'tp'), parts along dimension 0, may hold values from -9 to 9
- new_values: bfloat16 [4096, 1024], P('dp', 'tp'), parts along dimension 0, may hold values from -60 to 60
- cache_keys: bfloat16 [32, 32768, 128], P('dp', 'tp'), parts along dimension 0, may hold values from -4 to 4
- cache_values: bfloat16 [32, 32768, 128], P('dp', 'tp'), parts along dimension 0, may hold values from -60 to 60
- out_weight: bfloat16 [8192, 8192], P('tp'), may hold values from -0.09375 to 0.09375
- residual: bfloat16 [4096, 8192], P('dp', 'tp'), parts along dimension 0, may hold values from -8 to 8
- norm_gain: bfloat16 [8192], P('tp'), may hold values from 0.5 to 1.5
Outputs:
- normed: bfloat16 [4096, 8192], P('dp', 'tp'), parts along dimension 0
The draws below stay inside these ranges and needn't reach their ends.
There are 8 independent parts, one for each index of `dp`. The reference program is written for one: setup_inputs(seed, part) draws one part's arguments, and reference() takes and returns one part's arrays. A program takes and returns all parts, laid end to end along the dimension named above; an argument that names none is the same for every part. Nothing has to cross between parts.
All inputs are finite; a program needn't handle non-finite values.
Results may differ from the reference program's by a relative error of at most 0.015.
Values may be sent and summed in bfloat16 or wider, within the bound.
A program may use at most 256 MiB of HBM per device.

```python
import math
import jax
import jax.numpy as jnp
from jax import lax

D = 8192
H = 64
KVH = 8
HD = 128
SPAN = 128
SEQS = 4
CTX = 4096
TOK = 512


def build_drawn(key):
    key_stored = jax.random.fold_in(key, 11)
    key_query = jax.random.fold_in(key, 12)
    stored = jax.random.truncated_normal(key_stored, -4.0, 4.0, (SEQS, KVH * CTX, HD), jnp.float32)
    asked = jax.random.truncated_normal(key_query, -4.0, 4.0, (SEQS * SPAN, H * HD), jnp.float32)
    return (stored, asked)


def draw_cache_keys(key, part):
    return build_drawn(key)[0].astype(jnp.bfloat16)


def draw_queries(key, part):
    return build_drawn(key)[1].astype(jnp.bfloat16)


def draw_residual(key, part):
    key_base = jax.random.fold_in(key, 21)
    position = jnp.arange(D, dtype=jnp.float32) / D
    rising = 0.15 * jnp.exp(position * math.log(3.0))
    values = jax.random.truncated_normal(key_base, -4.0, 4.0, (SEQS * SPAN, D), jnp.float32) * rising[None, :]
    return values.astype(jnp.bfloat16)


def spiked(values, own_key, source, target, parts, factor):
    owner, partner = [(jnp.arange(values.shape[dim]) // (values.shape[dim] // parts)).reshape([-1 if axis == dim else 1 for axis in range(values.ndim)]) for dim in (source, target)]
    chosen = jax.random.permutation(own_key, parts)[partner]
    strong = (owner == chosen) | (owner == (partner + parts // 2) % parts)
    return jnp.where(strong, factor * values, values)


def levels(own_key, shape, shards, low, high):
    factor_of = 1.0
    for dim, parts in shards:
        draws = jax.random.uniform(jax.random.fold_in(jax.random.fold_in(own_key, 6), dim), (parts,), jnp.float32, low / len(shards), high / len(shards))
        factor_of = factor_of * jnp.repeat(jnp.exp(draws), shape[dim] // parts).reshape((-1,) + (1,) * (len(shape) - 1 - dim))
    return factor_of


def scatter_about(own_key, shape, deviation, limit, split=(), held_as=jnp.bfloat16):
    drawn = jax.random.normal(own_key, shape, jnp.float32) * deviation
    if len(split) > 0:
        drawn = levels(own_key, shape, split, -0.22, 0.18) * drawn
    return jnp.clip(drawn, min=-limit, max=limit).astype(held_as)


def heavy_noise(stream_key, extent, spread, most, pieces, heavy, held_as=jnp.bfloat16):
    values = spread * jax.random.normal(stream_key, extent, jnp.float32)
    if pieces:
        values = values * levels(stream_key, extent, pieces, -0.22, 0.18)
    return jnp.clip(spiked(values, jax.random.fold_in(stream_key, 3), *heavy), -most, most).astype(held_as)


def setup_inputs(seed: int = 0, part: int = 0) -> dict:
    keys = jax.random.split(jax.random.key(seed), 9)
    part_splits = jax.random.split(jax.random.fold_in(keys[8], part), 9)
    queries = draw_queries(jax.random.fold_in(jax.random.fold_in(keys[8], part), 71), part)
    new_keys = scatter_about(part_splits[1], (TOK, KVH * HD), 1.5, 9.0, ((1, 4),))
    new_values = scatter_about(part_splits[2], (TOK, KVH * HD), 10.0, 60.0, ((1, 4),))
    cache_keys = draw_cache_keys(jax.random.fold_in(jax.random.fold_in(keys[8], part), 71), part)
    cache_values = scatter_about(part_splits[4], (SEQS, KVH * CTX, HD), 10.0, 60.0, ((1, 4),))
    out_weight = heavy_noise(keys[5], (H * HD, D), (H * HD) ** -0.5, 0.09375, ((0, 4),), (0, 1, 4, 2.0))
    residual = draw_residual(jax.random.fold_in(jax.random.fold_in(keys[8], part), 71), part)
    norm_gain = jnp.clip(1.0 + 0.1 * jax.random.normal(keys[7], (D,), jnp.float32), 0.5, 1.5).astype(jnp.bfloat16)
    return {"queries": queries, "new_keys": new_keys, "new_values": new_values, "cache_keys": cache_keys, "cache_values": cache_values, "out_weight": out_weight, "residual": residual, "norm_gain": norm_gain}


def attend_sequence(inputs):
    query_rows, fresh_keys, fresh_values, stored_keys, stored_values = inputs
    groups = H // KVH
    scaling = HD ** (-0.5)
    grouped = query_rows.astype(jnp.float32).reshape(SPAN, KVH, groups, HD)
    old_keys = stored_keys.astype(jnp.float32).reshape(KVH, CTX, HD)
    old_values = stored_values.astype(jnp.float32).reshape(KVH, CTX, HD)
    recent_keys = fresh_keys.astype(jnp.float32).reshape(SPAN, KVH, HD)
    recent_values = fresh_values.astype(jnp.float32).reshape(SPAN, KVH, HD)
    old_scores = jnp.einsum('ighd,gjd->ghij', grouped, old_keys) * scaling
    recent_scores = jnp.einsum('ighd,jgd->ghij', grouped, recent_keys) * scaling
    causal = jnp.arange(SPAN)[:, None] >= jnp.arange(SPAN)[None, :]
    recent_scores = jnp.where(causal, recent_scores, -jnp.inf)
    peak = jnp.maximum(lax.optimization_barrier(jnp.max(old_scores, axis=-1)), lax.optimization_barrier(jnp.max(recent_scores, axis=-1)))
    old_weights = jnp.exp(old_scores - peak[..., None])
    recent_weights = jnp.exp(recent_scores - peak[..., None])
    total = lax.optimization_barrier(jnp.sum(old_weights, axis=-1)) + lax.optimization_barrier(jnp.sum(recent_weights, axis=-1))
    rounded_old = lax.optimization_barrier(old_weights.astype(jnp.bfloat16)).astype(jnp.float32)
    rounded_recent = lax.optimization_barrier(recent_weights.astype(jnp.bfloat16)).astype(jnp.float32)
    mixed = jnp.einsum('ghij,gjd->ighd', rounded_old, old_values)
    mixed = mixed + jnp.einsum('ghij,jgd->ighd', rounded_recent, recent_values)
    result = mixed / jnp.transpose(total, (2, 0, 1))[..., None]
    return result.reshape(SPAN, H * HD).astype(jnp.bfloat16)

def reference(queries, new_keys, new_values, cache_keys, cache_values, out_weight, residual, norm_gain):
    inputs = (queries.reshape(SEQS, SPAN, H * HD), new_keys.reshape(SEQS, SPAN, KVH * HD), new_values.reshape(SEQS, SPAN, KVH * HD), cache_keys, cache_values)
    attended = lax.map(attend_sequence, inputs).reshape(SEQS * SPAN, H * HD)
    projected = jnp.dot(attended, out_weight, preferred_element_type=jnp.float32)
    hidden = residual.astype(jnp.float32) + projected
    power = lax.optimization_barrier(jnp.mean(hidden * hidden, axis=1, keepdims=True))
    normed = hidden * lax.rsqrt(power + 1e-05) * norm_gain.astype(jnp.float32)
    return normed.astype(jnp.bfloat16)
```

```python
import functools

import jax
import jax.numpy as jnp
from jax import lax
from jax.experimental import pallas as pl
from jax.experimental.pallas import tpu as pltpu
from jax.sharding import PartitionSpec as P

D = 8192
KVH = 8
HD = 128
SPAN = 128
SEQS = 4
CTX = 4096


EPSILON = 1e-05


def partner(value, axis, bit):
    mask = 2**bit
    pairs = [(source, source ^ mask) for source in range(lax.axis_size(axis))]
    return lax.ppermute(value, axis, pairs)


def attend_block(query_rows, stored_keys, stored_values, fresh_keys, fresh_values, local_kv):
    heads_here = query_rows.shape[1] // HD
    groups = heads_here // local_kv
    length = stored_keys.shape[1] // local_kv
    scaling = HD ** (-0.5)
    grouped = query_rows.reshape(SEQS, SPAN, local_kv, groups, HD)
    old_keys = stored_keys.reshape(SEQS, local_kv, length, HD)
    old_values = stored_values.reshape(SEQS, local_kv, length, HD)
    scores = (
        jnp.einsum("sighd,sgjd->sghij", grouped, old_keys, preferred_element_type=jnp.float32)
        * scaling
    )
    peak = jnp.max(scores, axis=-1)
    recent_keys = fresh_keys.reshape(SEQS, SPAN, local_kv, HD)
    recent_values = fresh_values.reshape(SEQS, SPAN, local_kv, HD)
    recent_scores = (
        jnp.einsum("sighd,sjgd->sghij", grouped, recent_keys, preferred_element_type=jnp.float32)
        * scaling
    )
    causal = jnp.arange(SPAN)[:, None] >= jnp.arange(SPAN)[None, :]
    recent_scores = jnp.where(causal, recent_scores, -jnp.inf)
    peak = jnp.maximum(peak, jnp.max(recent_scores, axis=-1))
    weights = jnp.exp(scores - peak[..., None])
    total = jnp.sum(weights, axis=-1)
    mixed = jnp.einsum(
        "sghij,sgjd->sighd",
        weights.astype(jnp.bfloat16),
        old_values,
        preferred_element_type=jnp.float32,
    )
    recent_weights = jnp.exp(recent_scores - peak[..., None])
    total = total + jnp.sum(recent_weights, axis=-1)
    mixed = mixed + jnp.einsum(
        "sghij,sjgd->sighd",
        recent_weights.astype(jnp.bfloat16),
        recent_values,
        preferred_element_type=jnp.float32,
    )
    return (mixed, peak, total)


def token_layout(stat):
    return jnp.transpose(stat, (0, 3, 1, 2))[..., None]


def finish_rows(mixed, total):
    result = mixed / token_layout(total)
    return result.reshape(SEQS * SPAN, -1).astype(jnp.bfloat16)


def per_device(
    queries, new_keys, new_values, cache_keys, cache_values, out_weight, residual, norm_gain
):
    tp_size = lax.axis_size("tp")
    paired = tp_size == 2 * KVH
    local_kv = 1 if paired else cache_keys.shape[1] // CTX
    parity = lax.axis_index("tp") % 2

    def join_dims(own_piece, other_piece):
        first = jnp.concatenate([own_piece, other_piece], axis=-1)
        second = jnp.concatenate([other_piece, own_piece], axis=-1)
        return jnp.where(parity == 0, first, second)

    if paired:
        other_keys, other_values, other_stored_keys, other_stored_values = partner(
            (new_keys, new_values, cache_keys, cache_values), "tp", 0
        )
        fresh_keys = join_dims(new_keys, other_keys)
        fresh_values = join_dims(new_values, other_values)
        stored_keys = jnp.concatenate([cache_keys, other_stored_keys], axis=1)
        stored_values = jnp.concatenate([cache_values, other_stored_values], axis=1)
    else:
        fresh_keys, fresh_values = (new_keys, new_values)
        stored_keys, stored_values = (cache_keys, cache_values)
    mixed, peak, total = attend_block(
        queries, stored_keys, stored_values, fresh_keys, fresh_values, local_kv
    )
    attended = finish_rows(mixed, total)
    projected = lax.psum_scatter(
        lax.dot_general(
            out_weight, attended, (((0,), (1,)), ((), ())), preferred_element_type=jnp.float32
        ).astype(jnp.bfloat16),
        "tp",
        scatter_dimension=0,
        tiled=True,
    ).astype(jnp.float32)
    hidden = residual.astype(jnp.float32) + jnp.transpose(projected)
    squares = lax.psum(jnp.sum(hidden * hidden, axis=1), "tp")
    scaled = (
        hidden * lax.rsqrt(squares / D + EPSILON)[:, None] * norm_gain.astype(jnp.float32)[None, :]
    )
    return scaled.astype(jnp.bfloat16)


SEQS_PER_PART = 1
HEADS_PER_BLOCK = 2
KEY_CHUNK = 1024
PIECES = 4
MASKED = -1e30
LOG2E = 1.4426950408889634
MESH = pl.DeviceIdType.MESH


def lane_max(tile, running):
    for start in range(0, tile.shape[1], 128):
        part = tile[:, start : start + 128]
        running = part if running is None else jnp.maximum(running, part)
    return running


def attend_step(row, q_ref, k_ref, v_ref, nk_ref, nv_ref, att_ref, vx_ref, slots, column):
    stored = k_ref.shape[1]
    groups = q_ref.shape[1] // HD
    rows = HEADS_PER_BLOCK * SPAN
    blocks = groups // HEADS_PER_BLOCK
    vx_ref[0:stored, 0:HD] = v_ref[0]
    vx_ref[stored : stored + SPAN, 0:HD] = nv_ref[...]
    factor = HD ** (-0.5) * LOG2E
    chunks = [(start, KEY_CHUNK) for start in range(0, stored, KEY_CHUNK)] + [(stored, SPAN)]
    position = lax.broadcasted_iota(jnp.int32, (SPAN, SPAN), 0)
    causal_one = position >= lax.broadcasted_iota(jnp.int32, (SPAN, SPAN), 1)
    causal = jnp.concatenate([causal_one] * HEADS_PER_BLOCK, axis=0)

    def score_chunk(block, start, size, running):
        first = block * HEADS_PER_BLOCK
        heads = [q_ref[:, (first + i) * HD : (first + i + 1) * HD] for i in range(HEADS_PER_BLOCK)]
        q = heads[0] if len(heads) == 1 else jnp.concatenate(heads, axis=0)
        keys = nk_ref[...] if start == stored else k_ref[0, start : start + size, :]
        tile = lax.dot_general(
            q, keys, (((1,), (1,)), ((), ())), preferred_element_type=jnp.float32
        )
        if start == stored:
            tile = jnp.where(causal, tile, MASKED)
        slots[block % 2][:, start : start + size] = tile
        return lane_max(tile, running)

    running = None
    for start, size in chunks:
        running = score_chunk(0, start, size, running)
    for block in range(blocks):
        peak = jnp.max(running, axis=1, keepdims=True)
        running = None
        total = None
        for start, size in chunks:
            if block + 1 < blocks:
                running = score_chunk(block + 1, start, size, running)
            weights = jnp.exp2((slots[block % 2][:, start : start + size] - peak) * factor)
            term = jnp.dot(
                weights.astype(jnp.bfloat16),
                vx_ref[start : start + size, :],
                preferred_element_type=jnp.float32,
            )
            total = term if total is None else total + term
        result = (total[:, :HD] / total[:, HD:]).astype(jnp.bfloat16)
        for i in range(HEADS_PER_BLOCK):
            where = column + (block * HEADS_PER_BLOCK + i) * HD
            att_ref[pl.ds(row, SPAN), pl.ds(where, HD)] = result[i * SPAN : (i + 1) * SPAN]


def fused_kernel(
    q_ref, k_ref, v_ref, nk_ref, nv_ref, w_hbm, res_ref, gain_ref, out_hbm,
    w_ref, att_ref, vx_ref, score_a, score_b,
    s1_send, s1_recv, s2_send, s2_recv, hidden, staged, sq_send, sq_recv,
    w_sem, s1_ss, s1_rs, s2_ss, s2_rs, sq_ss, sq_rs, out_sem,
):
    s, g = pl.program_id(0), pl.program_id(1)
    local_kv = pl.num_programs(1)
    parts = SEQS // SEQS_PER_PART
    tokens = SEQS_PER_PART * SPAN
    width = hidden.shape[2]
    piece = width // PIECES
    me = lax.axis_index("tp")
    chip, core = me // 2, me % 2
    sibling = chip * 2 + (1 - core)
    across = (1 - chip) * 2 + core
    diagonal = (1 - chip) * 2 + (1 - core)
    w_pieces = w_sem.shape[0]
    w_rows = w_ref.shape[0] // w_pieces

    def w_copy(i):
        span = pl.ds(i * w_rows, w_rows)
        return pltpu.make_async_copy(w_hbm.at[span], w_ref.at[span], w_sem.at[i])

    def remote(src, dst, ss, rs, device):
        return pltpu.make_async_remote_copy(
            src_ref=src, dst_ref=dst, send_sem=ss, recv_sem=rs,
            device_id={"tp": device}, device_id_type=MESH,
        )

    def stage1(p, which, j):
        col = pl.ds(which * width + j * piece, piece)
        k = which * PIECES + j
        return remote(
            s1_send.at[:, col], s1_recv.at[p % 2, :, col], s1_ss.at[k], s1_rs.at[p % 2, k], sibling
        )

    def stage2(p, j):
        col = pl.ds(j * piece, piece)
        return remote(
            s2_send.at[:, col], s2_recv.at[p % 2, :, col], s2_ss.at[j], s2_rs.at[p % 2, j], across
        )

    def squares(p):
        return [
            remote(sq_send.at[p], sq_recv.at[p, i], sq_ss.at[p, i], sq_rs.at[p, i], device)
            for i, device in enumerate((sibling, across, diagonal))
        ]

    def out_copy(p):
        return pltpu.make_async_copy(
            staged.at[p % 2], out_hbm.at[pl.ds(p * tokens, tokens)], out_sem.at[p % 2]
        )

    @pl.when((s == 0) & (g == 0))
    def _():
        barrier = pltpu.get_barrier_semaphore()
        for device in (sibling, across, diagonal):
            pl.semaphore_signal(barrier, inc=1, device_id={"tp": device}, device_id_type=MESH)
        for i in range(w_pieces):
            w_copy(i).start()
        vx_ref[:, HD:] = jnp.ones((vx_ref.shape[0], vx_ref.shape[1] - HD), jnp.bfloat16)
        pl.semaphore_wait(barrier, 3)

    attend_step(
        pl.multiple_of(lax.rem(s, SEQS_PER_PART) * SPAN, SPAN),
        q_ref, k_ref, v_ref, nk_ref, nv_ref, att_ref, vx_ref, (score_a, score_b),
        pl.multiple_of(g * q_ref.shape[1], 128),
    )

    def project(owner, j):
        col = pl.multiple_of(owner * width + j * piece, 128)
        return jnp.dot(
            att_ref[...], w_ref[:, pl.ds(col, piece)], preferred_element_type=jnp.float32
        )

    def project_part(p):
        for j in range(PIECES):
            s1_send[:, j * piece : (j + 1) * piece] = project(diagonal, j).astype(jnp.bfloat16)
            stage1(p, 0, j).start()
            own = project(across, j)
            stage1(p, 0, j).wait_recv()
            both = own + s1_recv[p % 2, :, j * piece : (j + 1) * piece].astype(jnp.float32)
            s2_send[:, j * piece : (j + 1) * piece] = both.astype(jnp.bfloat16)
            stage2(p, j).start()
        for j in range(PIECES):
            col = slice(width + j * piece, width + (j + 1) * piece)
            s1_send[:, col] = project(sibling, j).astype(jnp.bfloat16)
            stage1(p, 1, j).start()
            own = slice(j * piece, (j + 1) * piece)
            hidden[p % 2, :, own] = project(me, j) + res_ref[:, own].astype(jnp.float32)

    def collect(p):
        for j in range(PIECES):
            stage1(p, 0, j).wait_send()
            stage1(p, 1, j).wait()
        lanes = None
        for j in range(PIECES):
            stage2(p, j).wait()
            col = slice(j * piece, (j + 1) * piece)
            other = slice(width + j * piece, width + (j + 1) * piece)
            value = (
                hidden[p % 2, :, col]
                + s1_recv[p % 2, :, other].astype(jnp.float32)
                + s2_recv[p % 2, :, col].astype(jnp.float32)
            )
            hidden[p % 2, :, col] = value
            for start in range(0, piece, 128):
                tile = value[:, start : start + 128]
                lanes = tile * tile if lanes is None else lanes + tile * tile
        for i in range(SEQS_PER_PART):
            turned = jnp.transpose(lanes[i * SPAN : (i + 1) * SPAN])
            row = jnp.sum(turned, axis=0, keepdims=True)
            sq_send[p, :, i * SPAN : (i + 1) * SPAN] = jnp.broadcast_to(row, (8, SPAN))
        for copy in squares(p):
            copy.start()

    def finish(p):
        for copy in squares(p):
            copy.wait()
        summed = sq_send[p] + sq_recv[p, 0] + sq_recv[p, 1] + sq_recv[p, 2]
        for i in range(SEQS_PER_PART):
            row = summed[0:1, i * SPAN : (i + 1) * SPAN]
            power = jnp.transpose(jnp.broadcast_to(row, (SPAN, SPAN))) / D
            scale = lax.rsqrt(power + EPSILON)
            for start in range(0, width, 128):
                value = hidden[p % 2, i * SPAN : (i + 1) * SPAN, start : start + 128]
                scaled = value * scale * gain_ref[:, start : start + 128].astype(jnp.float32)
                staged[p % 2, i * SPAN : (i + 1) * SPAN, start : start + 128] = scaled.astype(
                    jnp.bfloat16
                )
        out_copy(p).start()

    p = s // SEQS_PER_PART

    @pl.when((lax.rem(s, SEQS_PER_PART) == SEQS_PER_PART - 1) & (g == local_kv - 1))
    def _():
        @pl.when(p == 0)
        def _():
            for i in range(w_pieces):
                w_copy(i).wait()

        @pl.when(p > 0)
        def _():
            collect(p - 1)

        project_part(p)

        @pl.when(p > 2)
        def _():
            out_copy(p - 3).wait()

        @pl.when(p > 0)
        def _():
            finish(p - 1)

        @pl.when(p == parts - 1)
        def _():
            collect(p)
            if parts > 2:
                out_copy(p - 2).wait()
            finish(p)
            if parts > 1:
                out_copy(p - 1).wait()
            out_copy(p).wait()


def fused(queries, new_keys, new_values, cache_keys, cache_values, out_weight, residual, norm_gain):
    length = cache_keys.shape[1] // (new_keys.shape[1] // HD)
    local_kv = new_keys.shape[1] // HD
    group_width = queries.shape[1] // local_kv
    width = residual.shape[1]
    parts = SEQS // SEQS_PER_PART
    tokens = SEQS_PER_PART * SPAN
    keys_all = length + SPAN
    rows = HEADS_PER_BLOCK * SPAN
    bf16, f32 = jnp.bfloat16, jnp.float32
    dma = pltpu.SemaphoreType.DMA
    return pl.pallas_call(
        fused_kernel,
        grid=(SEQS, local_kv),
        out_shape=jax.ShapeDtypeStruct(residual.shape, bf16),
        in_specs=[
            pl.BlockSpec((SPAN, group_width), lambda s, g: (s, g)),
            pl.BlockSpec((1, length, HD), lambda s, g: (s, g, 0)),
            pl.BlockSpec((1, length, HD), lambda s, g: (s, g, 0)),
            pl.BlockSpec((SPAN, HD), lambda s, g: (s, g)),
            pl.BlockSpec((SPAN, HD), lambda s, g: (s, g)),
            pl.BlockSpec(memory_space=pl.ANY),
            pl.BlockSpec((tokens, width), lambda s, g: (s // SEQS_PER_PART, 0)),
            pl.BlockSpec((1, width), lambda s, g: (0, 0)),
        ],
        out_specs=pl.BlockSpec(memory_space=pl.ANY),
        scratch_shapes=[
            pltpu.VMEM(out_weight.shape, bf16),
            pltpu.VMEM((tokens, queries.shape[1]), bf16),
            pltpu.VMEM((keys_all, 2 * HD), bf16),
            pltpu.VMEM((rows, keys_all), f32),
            pltpu.VMEM((rows, keys_all), f32),
            pltpu.VMEM((tokens, 2 * width), bf16),
            pltpu.VMEM((2, tokens, 2 * width), bf16),
            pltpu.VMEM((tokens, width), bf16),
            pltpu.VMEM((2, tokens, width), bf16),
            pltpu.VMEM((2, tokens, width), f32),
            pltpu.VMEM((2, tokens, width), bf16),
            pltpu.VMEM((parts, 8, tokens), f32),
            pltpu.VMEM((parts, 3, 8, tokens), f32),
            dma((8,)),
            dma((2 * PIECES,)),
            dma((2, 2 * PIECES)),
            dma((PIECES,)),
            dma((2, PIECES)),
            dma((parts, 3)),
            dma((parts, 3)),
            dma((2,)),
        ],
        compiler_params=pltpu.CompilerParams(
            collective_id=0,
            has_side_effects=True,
            vmem_limit_bytes=67043328,
            dimension_semantics=("arbitrary", "arbitrary"),
        ),
    )(
        queries, cache_keys, cache_values, new_keys, new_values, out_weight, residual,
        norm_gain.reshape(1, -1),
    )


def solution(mesh):
    in_specs = (
        P("dp", "tp"),
        P("dp", "tp"),
        P("dp", "tp"),
        P("dp", "tp", None),
        P("dp", "tp", None),
        P("tp", None),
        P("dp", "tp"),
        P("tp"),
    )
    out_specs = P("dp", "tp")
    return jax.shard_map(
        fused if mesh.shape["tp"] == 4 else per_device, mesh=mesh, in_specs=in_specs, out_specs=out_specs, check_vma=False
    )
```
